256 devices in a mesh: pipe: 32 (over z, y_hi, core), ctx: 8 (over x, y_lo).
Axes of the slice: x: 4, y: 4 (y_hi: 2, y_lo: 2; y = y_hi * 2 + y_lo), z: 8, core: 2. Of those that a mesh axis runs over, the one named last changes fastest.
Arguments:
- query_fwd: bfloat16 [32, 1024, 4096], P('pipe', 'ctx'), may hold values from -110 to 110
- key_fwd: bfloat16 [32, 1024, 1024], P('pipe', 'ctx'), may hold values from -4.5 to 4.5
- value_fwd: bfloat16 [32, 1024, 1024], P('pipe', 'ctx'), may hold values from -6 to 6
- query_bwd: bfloat16 [32, 1024, 4096], P('pipe', 'ctx'), may hold values from -110 to 110
- key_bwd: bfloat16 [32, 1024, 1024], P('pipe', 'ctx'), may hold values from -4.5 to 4.5
- value_bwd: bfloat16 [32, 1024, 1024], P('pipe', 'ctx'), may hold values from -6 to 6
- cotangent: bfloat16 [32, 1024, 4096], P('pipe', 'ctx'), may hold values from -6 to 6
- documents: int32 [32, 2, 1024], P('pipe'), may hold values from 0 to 3, never falling along the last dimension, each value on 1 to 512 neighbouring positions
Outputs:
- attended: bfloat16 [32, 1024, 4096], P('pipe', 'ctx')
- query_grad: bfloat16 [32, 1024, 4096], P('pipe', 'ctx')
- key_grad: bfloat16 [32, 1024, 1024], P('pipe', 'ctx')
- value_grad: bfloat16 [32, 1024, 1024], P('pipe', 'ctx')
The draws below stay inside these ranges and needn't reach their ends.
Inputs may be any that keep to these rules, and one draw needn't show every extreme that they name: Along the last dimension ids never fall; 4 documents per slab, each of 1 to 512 positions, one of exactly 512.
All inputs are finite; a program needn't handle non-finite values.
Results may differ from the reference program's by a relative error of at most 0.0085.
Values may be sent and summed in bfloat16 or wider, within the bound.
No kernel may reach another device: no remote copies, remote signals or barrier semaphores. Data moves between devices by JAX's collectives and lax.ppermute only.
A program may use at most 128 MiB of HBM per device.

```python
import math
import jax
import jax.numpy as jnp
import numpy as np
from jax import lax

QHEADS = 32
KVH = 8
HD = 128
QBLK = 128
DOCS = 4
SEQ = 1024
SECTIONS = 32


def joint_draw(key, which):
    base = jax.random.fold_in(key, 101 + which)
    keys_drawn = jnp.clip(jax.random.normal(jax.random.fold_in(base, 1), (SECTIONS, SEQ, KVH, HD), jnp.float32), -4.0, 4.0)
    query_drawn = jnp.clip(jax.random.normal(jax.random.fold_in(base, 2), (SECTIONS, SEQ, KVH, QHEADS // KVH, HD), jnp.float32), -4.0, 4.0)
    return (query_drawn.reshape(SECTIONS, SEQ, QHEADS * HD), keys_drawn.reshape(SECTIONS, SEQ, KVH * HD))


def draw_query_fwd(key, part):
    return joint_draw(key, 0)[0].astype(jnp.bfloat16)


def draw_key_fwd(key, part):
    return joint_draw(key, 0)[1].astype(jnp.bfloat16)


def draw_query_bwd(key, part):
    return joint_draw(key, 1)[0].astype(jnp.bfloat16)


def draw_key_bwd(key, part):
    return joint_draw(key, 1)[1].astype(jnp.bfloat16)


def shard_levels(rng, dims, shards, smallest, high):
    level, own = 1.0, jax.random.fold_in(rng, 6)
    for dim, blocks in shards:
        steps = jnp.exp(jax.random.uniform(jax.random.fold_in(own, dim), (blocks,), jnp.float32, smallest / len(shards), high / len(shards)))
        level = level * jnp.repeat(steps, dims[dim] // blocks).reshape([-1 if axis == dim else 1 for axis in range(len(dims))])
    return level


def split_up(count, total, most, skew):
    portions = [(1 << 20) // math.isqrt(rank ** skew) + 1 for rank in range(2, count + 1)]
    rest, holding = total - most - (count - 1), [1] * (count - 1)
    while rest > 0:
        candidates = [i for i in range(count - 1) if holding[i] < most]
        pool, budget = sum([portions[i] for i in candidates]), rest
        for i in candidates:
            extra = min(most - holding[i], max(1, budget * portions[i] // pool), rest)
            holding[i] = holding[i] + extra
            rest = rest - extra
    return np.array([most] + holding)


def ragged_sizes(key, number_of, total, reach, slope):
    if number_of == 2:
        one = jax.random.randint(key, (), max(1, total - reach), min(reach, total - 1) + 1)
        return jnp.stack([one, total - one])
    lengths = jnp.asarray(split_up(number_of, total, reach, slope), jnp.int32)
    pairs = (number_of - 1) // 2
    donor, taker = lengths[1:1 + 2 * pairs:2], lengths[2:2 + 2 * pairs:2]
    margin = jnp.minimum(donor - 1, reach - taker)
    shifted = jax.random.randint(jax.random.fold_in(key, 1), (pairs,), 0, 1 << 20) % (margin + 1)
    lengths = lengths.at[1:1 + 2 * pairs:2].set(donor - shifted).at[2:2 + 2 * pairs:2].set(taker + shifted)
    return lengths[jax.random.permutation(jax.random.fold_in(key, 2), number_of)]


def bell_draw(key, shape, spread, reach, cuts=(), kind=jnp.bfloat16):
    result = jax.random.normal(key, shape, jnp.float32) * spread
    if len(cuts) > 0:
        result = shard_levels(key, shape, cuts, -0.22, 0.18) * result
    return jnp.clip(result, min=-reach, max=reach).astype(kind)


def setup_inputs(seed: int = 0) -> dict:
    seeds = jax.random.split(jax.random.key(seed), 9)
    return {
        "query_fwd": draw_query_fwd(jax.random.fold_in(seeds[8], 71), 0),
        "key_fwd": draw_key_fwd(jax.random.fold_in(seeds[8], 71), 0),
        "value_fwd": bell_draw(seeds[2], (SECTIONS, SEQ, KVH * HD), 1.0, 6.0, ((0, 32), (1, 8))),
        "query_bwd": draw_query_bwd(jax.random.fold_in(seeds[8], 71), 0),
        "key_bwd": draw_key_bwd(jax.random.fold_in(seeds[8], 71), 0),
        "value_bwd": bell_draw(seeds[5], (SECTIONS, SEQ, KVH * HD), 1.0, 6.0, ((0, 32), (1, 8))),
        "cotangent": bell_draw(seeds[6], (SECTIONS, SEQ, QHEADS * HD), 1.0, 6.0, ((0, 32), (1, 8))),
        "documents": jax.vmap(lambda own: jnp.searchsorted(jnp.cumsum(ragged_sizes(own, DOCS, SEQ, SEQ // 2, 1)), jnp.arange(SEQ), side="right"))(jax.random.split(seeds[7], SECTIONS * 2)).reshape((SECTIONS, 2, SEQ)).astype(jnp.int32),
    }


def allowed_mask(query_places, query_documents, key_places, key_documents):
    causal = key_places[None, :] <= query_places[:, None]
    same_document = key_documents[None, :] == query_documents[:, None]
    return causal & same_document


def head_probs(query_head, key_head, allowed, score_scale):
    raw_scores = jnp.einsum("rgd,kd->grk", query_head.astype(jnp.float32), key_head.astype(jnp.float32)) * score_scale
    masked = jnp.where(allowed[None], raw_scores, jnp.float32(-1e30))
    row_max = jnp.max(masked, axis=-1, keepdims=True)
    exponent = jnp.exp(masked - row_max)
    return exponent / jnp.sum(exponent, axis=-1, keepdims=True)


def forward_all(queries, keys_all, values_all, query_places, query_documents, key_places, key_documents):
    row_count, head_count, query_width = queries.shape
    head_size = keys_all.shape[2]
    score_scale = head_size ** -0.5
    block_count = row_count // QBLK
    query_blocks = queries.reshape(block_count, QBLK, head_count, query_width)
    place_blocks = query_places.reshape(block_count, QBLK)
    document_blocks = query_documents.reshape(block_count, QBLK)

    def one_block(packed):
        query_block, place_block, document_block = packed
        allowed = allowed_mask(place_block, document_block, key_places, key_documents)

        def one_head(head):
            query_head = lax.dynamic_index_in_dim(query_block, head, 1, False).reshape(QBLK, -1, head_size)
            key_head = lax.dynamic_index_in_dim(keys_all, head, 1, False)
            value_head = lax.dynamic_index_in_dim(values_all, head, 1, False)
            weights = head_probs(query_head, key_head, allowed, score_scale).astype(jnp.bfloat16)
            mixture = jnp.einsum("grk,kd->rgd", weights.astype(jnp.float32), value_head.astype(jnp.float32))
            return mixture.reshape(QBLK, query_width).astype(jnp.bfloat16)

        return jnp.moveaxis(lax.map(one_head, jnp.arange(head_count, dtype=jnp.int32)), 0, 1)

    outcome = lax.map(one_block, (query_blocks, place_blocks, document_blocks))
    return outcome.reshape(row_count, head_count, query_width)


def backward_all(queries, keys_all, values_all, cotan, query_places, query_documents, key_places, key_documents):
    row_count, head_count, query_width = queries.shape
    head_size = keys_all.shape[2]
    score_scale = head_size ** -0.5
    block_count = row_count // QBLK
    query_blocks = queries.reshape(block_count, QBLK, head_count, query_width)
    cotan_blocks = cotan.reshape(block_count, QBLK, head_count, query_width)
    place_blocks = query_places.reshape(block_count, QBLK)
    document_blocks = query_documents.reshape(block_count, QBLK)

    def one_block(totals, packed):
        query_block, cotan_block, place_block, document_block = packed
        allowed = allowed_mask(place_block, document_block, key_places, key_documents)

        def one_head(head):
            query_head = lax.dynamic_index_in_dim(query_block, head, 1, False).reshape(QBLK, -1, head_size)
            cotan_head = lax.dynamic_index_in_dim(cotan_block, head, 1, False).reshape(QBLK, -1, head_size)
            key_head = lax.dynamic_index_in_dim(keys_all, head, 1, False)
            value_head = lax.dynamic_index_in_dim(values_all, head, 1, False)
            probability = head_probs(query_head, key_head, allowed, score_scale)
            weights = probability.astype(jnp.bfloat16)
            prob_grad = jnp.einsum("rgd,kd->grk", cotan_head.astype(jnp.float32), value_head.astype(jnp.float32))
            row_delta = jnp.sum(probability * prob_grad, axis=-1, keepdims=True)
            score_grad = (probability * (prob_grad - row_delta) * score_scale).astype(jnp.bfloat16)
            query_part = jnp.einsum("grk,kd->rgd", score_grad.astype(jnp.float32), key_head.astype(jnp.float32))
            key_part = jnp.einsum("grk,rgd->kd", score_grad.astype(jnp.float32), query_head.astype(jnp.float32))
            value_part = jnp.einsum("grk,rgd->kd", weights.astype(jnp.float32), cotan_head.astype(jnp.float32))
            return query_part.reshape(QBLK, query_width).astype(jnp.bfloat16), key_part, value_part

        query_part, key_part, value_part = lax.map(one_head, jnp.arange(head_count, dtype=jnp.int32))
        new_totals = (totals[0] + jnp.moveaxis(key_part, 0, 1), totals[1] + jnp.moveaxis(value_part, 0, 1))
        return new_totals, jnp.moveaxis(query_part, 0, 1)

    empty_sum = jnp.zeros(keys_all.shape, jnp.float32)
    sums, query_grads = lax.scan(one_block, (empty_sum, empty_sum), (query_blocks, cotan_blocks, place_blocks, document_blocks))
    return query_grads.reshape(row_count, head_count, query_width), sums[0], sums[1]


def section_forward(packed):
    queries, keys_in, values_in, docs_row = packed
    places = jnp.arange(SEQ, dtype=jnp.int32)
    outcome = forward_all(queries.reshape(SEQ, KVH, -1), keys_in.reshape(SEQ, KVH, -1), values_in.reshape(SEQ, KVH, -1), places, docs_row, places, docs_row)
    return outcome.reshape(SEQ, -1)


def section_backward(packed):
    queries, keys_in, values_in, cotan, docs_row = packed
    places = jnp.arange(SEQ, dtype=jnp.int32)
    query_part, key_part, value_part = backward_all(queries.reshape(SEQ, KVH, -1), keys_in.reshape(SEQ, KVH, -1), values_in.reshape(SEQ, KVH, -1), cotan.reshape(SEQ, KVH, -1), places, docs_row, places, docs_row)
    return query_part.reshape(SEQ, -1), key_part.reshape(SEQ, -1).astype(jnp.bfloat16), value_part.reshape(SEQ, -1).astype(jnp.bfloat16)


def reference(query_fwd, key_fwd, value_fwd, query_bwd, key_bwd, value_bwd, cotangent, documents):
    attended = lax.map(section_forward, (jnp.roll(query_fwd, 1, 0), jnp.roll(key_fwd, 1, 0), jnp.roll(value_fwd, 1, 0), documents[:, 0]))
    query_part, key_part, value_part = lax.map(section_backward, (query_bwd, key_bwd, value_bwd, jnp.roll(cotangent, -1, 0), documents[:, 1]))
    return attended, jnp.roll(query_part, -1, 0), jnp.roll(key_part, -1, 0), jnp.roll(value_part, -1, 0)
```

```python
import jax
import jax.numpy as jnp
from jax import lax
from jax.experimental import pallas as pl
from jax.experimental.pallas import tpu as pltpu
from jax.sharding import PartitionSpec as P


QHEADS = 32
KVH = 8
HD = 128
QBLK = 128
SEQ = 1024
GROUP = QHEADS // KVH
XS = 4
SLAB_KV = KVH // XS
QW = SLAB_KV * GROUP * HD
KW = SLAB_KV * HD
REACH = 4
MASKED = -1e30
SCALE = HD**-0.5
EXP2_SCALE = SCALE * 1.4426950408889634
F32 = jnp.float32
BF16 = jnp.bfloat16


def nt(a, b):
    return lax.dot_general(a, b, (((1,), (1,)), ((), ())), preferred_element_type=F32)


def nn(a, b):
    return lax.dot_general(a, b, (((1,), (0,)), ((), ())), preferred_element_type=F32)


def tn(a, b):
    return lax.dot_general(a, b, (((0,), (0,)), ((), ())), preferred_element_type=F32)


def place():
    rank = lax.axis_index("ctx")
    return rank // 2, rank % 2


def vmem_call(body, outs, scratch=()):
    return pl.pallas_call(
        body,
        out_shape=outs,
        scratch_shapes=scratch,
        compiler_params=pltpu.CompilerParams(vmem_limit_bytes=20 * 1024 * 1024),
    )


def cut_body(*refs):
    in_refs, (out_ref, held_ref, in_sems, out_sems) = refs[:-4], refs[-4:]
    loads = []
    for slab in range(XS):
        at, row = 0, []
        for n, ref in enumerate(in_refs):
            width = ref.shape[2] // XS
            source = ref.at[0, :, slab * width : (slab + 1) * width]
            target = held_ref.at[slab, :, at : at + width]
            row.append(pltpu.make_async_copy(source, target, in_sems.at[slab, n]))
            at += width
        loads.append(row)
    for row in loads:
        for load in row:
            load.start()
    stores = []
    for slab, row in enumerate(loads):
        for load in row:
            load.wait()
        stores.append(
            pltpu.make_async_copy(held_ref.at[slab], out_ref.at[slab], out_sems.at[slab])
        )
        stores[-1].start()
    for store in stores:
        store.wait()


def cut(*arrays):
    width = sum(a.shape[2] for a in arrays) // XS
    shape = (XS, QBLK, width)
    return pl.pallas_call(
        cut_body,
        in_specs=[pl.BlockSpec(memory_space=pl.ANY)] * len(arrays),
        out_specs=pl.BlockSpec(memory_space=pl.ANY),
        out_shape=jax.ShapeDtypeStruct(shape, BF16),
        scratch_shapes=[
            pltpu.VMEM(shape, BF16),
            pltpu.SemaphoreType.DMA((XS, len(arrays))),
            pltpu.SemaphoreType.DMA((XS,)),
        ],
    )(*arrays)


def turned_body(in_ref, *refs):
    out_refs, sems = refs[:XS], refs[XS]
    x, _ = place()
    width = in_ref.shape[2] // XS
    loads = []
    for k in range(XS):
        start = pl.multiple_of(lax.rem(x + k, XS) * width, width)
        source = in_ref.at[0, :, pl.ds(start, width)]
        loads.append(pltpu.make_async_copy(source, out_refs[k], sems.at[k]))
        loads[-1].start()
    for load in loads:
        load.wait()


def turned(array):
    width = array.shape[2] // XS
    return pl.pallas_call(
        turned_body,
        in_specs=[pl.BlockSpec(memory_space=pl.ANY)],
        out_specs=[pl.BlockSpec(memory_space=pltpu.VMEM)] * XS,
        out_shape=[jax.ShapeDtypeStruct((QBLK, width), BF16)] * XS,
        scratch_shapes=[pltpu.SemaphoreType.DMA((XS,))],
    )(array)


def joined_body(*refs):
    x, _ = place()
    out_ref, width = refs[XS], refs[0].shape[1]
    for k in range(XS):
        start = pl.multiple_of(lax.rem(x - k + XS, XS) * width, width)
        out_ref[0, :, pl.ds(start, width)] = refs[k][...]


def joined(parts):
    width = parts[0].shape[1]
    return vmem_call(joined_body, jax.ShapeDtypeStruct((1, QBLK, XS * width), BF16))(*parts)


def joined_grads_body(*refs):
    x, _ = place()
    mine, theirs, (dq_ref, dk_ref, dv_ref) = refs[:XS], refs[XS : 2 * XS], refs[2 * XS :]
    for k in range(XS):
        slab = lax.rem(x - k + XS, XS)
        wide = pl.multiple_of(slab * QW, QW)
        start = pl.multiple_of(slab * KW, KW)
        dq_ref[0, :, pl.ds(wide, QW)] = mine[k][:, :QW]
        total = mine[k][:, QW:].astype(F32) + theirs[k][...].astype(F32)
        dk_ref[0, :, pl.ds(start, KW)] = total[:, :KW].astype(BF16)
        dv_ref[0, :, pl.ds(start, KW)] = total[:, KW:].astype(BF16)


def joined_grads(mine, theirs):
    shape = jax.ShapeDtypeStruct((1, QBLK, XS * KW), BF16)
    wide = jax.ShapeDtypeStruct((1, QBLK, XS * QW), BF16)
    return vmem_call(joined_grads_body, (wide, shape, shape))(*mine, *theirs)


def sent_turned(parts, steps, flip=0):
    count, outs = lax.axis_size("pipe"), []
    for k in range(XS):
        pairs = []
        for p in range(count):
            for c in range(2 * XS):
                target = (c // 2 + k) % XS * 2 + (c + flip) % 2
                pairs.append((p * 2 * XS + c, (p + steps) % count * 2 * XS + target))
        outs.append(lax.ppermute(parts[k], ("pipe", "ctx"), pairs))
    return outs


def across(value):
    return lax.ppermute(value, "ctx", [(c, c ^ 1) for c in range(2 * XS)])


def over_x(value):
    evens = [2 * x for x in range(XS)]
    odds = [2 * x + 1 for x in range(XS)]
    return lax.all_to_all(
        value, "ctx", split_axis=0, concat_axis=0, axis_index_groups=[evens, odds], tiled=True
    )


def window_of(i, y):
    blocks = min(2 * i + 2, REACH + 1)
    start = 0 if blocks <= REACH else (2 * i - REACH + y)
    return blocks * QBLK, start


def fill_window(y, base, own_ref, other_ref, k_ref, v_ref):
    for i in range(XS):
        own = pl.multiple_of((2 * i + y) * QBLK, QBLK)
        other = pl.multiple_of((2 * i + 1 - y) * QBLK, QBLK)
        k_ref[pl.ds(own, QBLK), :] = own_ref[i, :, base : base + KW]
        v_ref[pl.ds(own, QBLK), :] = own_ref[i, :, base + KW : base + 2 * KW]
        k_ref[pl.ds(other, QBLK), :] = other_ref[i, :, :KW]
        v_ref[pl.ds(other, QBLK), :] = other_ref[i, :, KW:]


def fill_docs(docs_ref, which, col_ref, row_ref):
    for b in range(SEQ // QBLK):
        row = docs_ref[0, which : which + 1, b * QBLK : (b + 1) * QBLK].astype(F32)
        row_ref[b] = jnp.broadcast_to(row, (8, QBLK))
        col_ref[b * QBLK : (b + 1) * QBLK, :] = jnp.broadcast_to(row, (QBLK, QBLK)).T


def fill_bias(i, y, col_ref, row_ref, bias_ref):
    length, start = window_of(i, y)
    first = pl.multiple_of(start * QBLK, QBLK)
    key_docs = col_ref[pl.ds(first, length), :]
    query_docs = row_ref[2 * i + y][:1]
    key_places = first + lax.broadcasted_iota(jnp.int32, (length, QBLK), 0)
    query_places = (2 * i + y) * QBLK + lax.broadcasted_iota(jnp.int32, (length, QBLK), 1)
    seen = (key_places <= query_places) & (key_docs == query_docs)
    bias_ref[:length, :] = jnp.where(seen, F32(0), F32(MASKED))


def stacked(ref, i, base):
    return jnp.concatenate(
        [ref[i, :, base + h * HD : base + (h + 1) * HD] for h in range(GROUP)], axis=0
    )


def probs_of(scores, bias):
    masked = scores + jnp.concatenate([bias] * GROUP, axis=1)
    row_max = jnp.max(masked, axis=0, keepdims=True)
    exponent = jnp.exp2((masked - row_max) * F32(EXP2_SCALE))
    return exponent * (1.0 / jnp.sum(exponent, axis=0, keepdims=True))


def forward_body(q0, q1, q2, q3, own_ref, other_ref, docs_ref, *refs):
    out_refs, (q_ref, mixed_ref, k_ref, v_ref, col_ref, row_ref, bias_ref) = refs[:XS], refs[XS:]
    x, y = place()
    for k, chunk in enumerate((q0, q1, q2, q3)):
        q_ref[lax.rem(x - k + XS, XS)] = chunk[...]
    fill_window(y, 2 * KW, own_ref, other_ref, k_ref, v_ref)
    fill_docs(docs_ref, 0, col_ref, row_ref)
    for i in range(XS):
        length, start = window_of(i, y)
        first = pl.multiple_of(start * QBLK, QBLK)
        fill_bias(i, y, col_ref, row_ref, bias_ref)
        for g in range(SLAB_KV):
            keys = k_ref[pl.ds(first, length), g * HD : (g + 1) * HD]
            values = v_ref[pl.ds(first, length), g * HD : (g + 1) * HD]
            queries = stacked(q_ref, i, g * GROUP * HD)
            weights = probs_of(nt(keys, queries), bias_ref[:length, :]).astype(BF16)
            mixed = tn(values, weights)
            for h in range(GROUP):
                col = (g * GROUP + h) * HD
                part = mixed[:, h * QBLK : (h + 1) * QBLK].T
                mixed_ref[i, :, col : col + HD] = part.astype(BF16)
    for k in range(XS):
        out_refs[k][...] = mixed_ref[lax.rem(x + k, XS)]


def forward(q, own, other, docs):
    return vmem_call(
        forward_body,
        (jax.ShapeDtypeStruct((QBLK, QW), BF16),) * XS,
        (
            pltpu.VMEM((XS, QBLK, QW), BF16),
            pltpu.VMEM((XS, QBLK, QW), BF16),
            pltpu.VMEM((SEQ, KW), BF16),
            pltpu.VMEM((SEQ, KW), BF16),
            pltpu.VMEM((SEQ, QBLK), F32),
            pltpu.VMEM((SEQ // QBLK, 8, QBLK), F32),
            pltpu.VMEM(((REACH + 1) * QBLK, QBLK), F32),
        ),
    )(*q, own, other, docs)


def backward_body(q_ref, g0, g1, g2, g3, own_ref, other_ref, docs_ref, *refs):
    mine_refs, theirs_refs = refs[:XS], refs[XS : 2 * XS]
    g_ref, dq_ref, k_ref, v_ref, col_ref, row_ref, bias_ref, dk_ref, dv_ref = refs[2 * XS :]
    x, y = place()
    for k, chunk in enumerate((g0, g1, g2, g3)):
        g_ref[lax.rem(x - k + XS, XS)] = chunk[...]
    fill_window(y, 0, own_ref, other_ref, k_ref, v_ref)
    fill_docs(docs_ref, 1, col_ref, row_ref)
    dk_ref[...] = jnp.zeros_like(dk_ref)
    dv_ref[...] = jnp.zeros_like(dv_ref)
    for i in range(XS):
        length, start = window_of(i, y)
        first = pl.multiple_of(start * QBLK, QBLK)
        fill_bias(i, y, col_ref, row_ref, bias_ref)
        for g in range(SLAB_KV):
            span = (pl.ds(first, length), slice(g * HD, (g + 1) * HD))
            keys, values = k_ref[span], v_ref[span]
            queries = stacked(q_ref, i, g * GROUP * HD)
            cotan = stacked(g_ref, i, g * GROUP * HD)
            probs = probs_of(nt(keys, queries), bias_ref[:length, :])
            prob_grad = nt(values, cotan)
            delta = jnp.sum(probs * prob_grad, axis=0, keepdims=True)
            score_grad = (probs * (prob_grad - delta) * F32(SCALE)).astype(BF16)
            dv_ref[span] += nn(probs.astype(BF16), cotan)
            dk_ref[span] += nn(score_grad, queries)
            dq = tn(keys, score_grad)
            for h in range(GROUP):
                col = (g * GROUP + h) * HD
                part = dq[:, h * QBLK : (h + 1) * QBLK].T
                dq_ref[i, :, col : col + HD] = part.astype(BF16)
    for k in range(XS):
        i = lax.rem(x + k, XS)
        own = pl.multiple_of((2 * i + y) * QBLK, QBLK)
        other = pl.multiple_of((2 * i + 1 - y) * QBLK, QBLK)
        mine_refs[k][:, :QW] = dq_ref[i]
        mine_refs[k][:, QW : QW + KW] = dk_ref[pl.ds(own, QBLK), :].astype(BF16)
        mine_refs[k][:, QW + KW :] = dv_ref[pl.ds(own, QBLK), :].astype(BF16)
        theirs_refs[k][:, :KW] = dk_ref[pl.ds(other, QBLK), :].astype(BF16)
        theirs_refs[k][:, KW:] = dv_ref[pl.ds(other, QBLK), :].astype(BF16)


def backward(q, g, own, other, docs):
    outs = vmem_call(
        backward_body,
        (jax.ShapeDtypeStruct((QBLK, QW + 2 * KW), BF16),) * XS
        + (jax.ShapeDtypeStruct((QBLK, 2 * KW), BF16),) * XS,
        (
            pltpu.VMEM((XS, QBLK, QW), BF16),
            pltpu.VMEM((XS, QBLK, QW), BF16),
            pltpu.VMEM((SEQ, KW), BF16),
            pltpu.VMEM((SEQ, KW), BF16),
            pltpu.VMEM((SEQ, QBLK), F32),
            pltpu.VMEM((SEQ // QBLK, 8, QBLK), F32),
            pltpu.VMEM(((REACH + 1) * QBLK, QBLK), F32),
            pltpu.VMEM((SEQ, KW), F32),
            pltpu.VMEM((SEQ, KW), F32),
        ),
    )(q, *g, own, other, docs)
    return outs[:XS], outs[XS:]


def shifted(value, steps):
    count = lax.axis_size("pipe")
    return lax.ppermute(value, "pipe", [(p, (p + steps) % count) for p in range(count)])


def on_device(query_fwd, key_fwd, value_fwd, query_bwd, key_bwd, value_bwd, cotangent, documents):
    own = over_x(cut(key_bwd, value_bwd, key_fwd, value_fwd))
    cotan = sent_turned(turned(cotangent), -1)
    docs_fwd = shifted(documents, -1)
    kv_bwd = across(own[:, :, : 2 * KW])
    kv_fwd = across(own[:, :, 2 * KW :])
    queries_bwd = over_x(cut(query_bwd))
    queries_fwd = sent_turned(turned(query_fwd), 0)
    mine, theirs = backward(queries_bwd, cotan, own, kv_bwd, documents)
    mine = sent_turned(mine, -1)
    theirs = sent_turned(theirs, -1, 1)
    mixed = forward(queries_fwd, own, kv_fwd, docs_fwd)
    mixed = sent_turned(mixed, 1)
    return joined(mixed), *joined_grads(mine, theirs)


def solution(mesh):
    rows = P("pipe", "ctx", None)
    return jax.shard_map(
        on_device,
        mesh=mesh,
        in_specs=(rows,) * 7 + (P("pipe", None, None),),
        out_specs=(rows,) * 4,
        check_vma=False,
    )
```

```python
import jax
import jax.numpy as jnp
from jax import lax
from jax.experimental import pallas as pl
from jax.experimental.pallas import tpu as pltpu
from jax.sharding import PartitionSpec as P


QHEADS = 32
KVH = 8
HD = 128
QBLK = 128
SEQ = 1024
GROUP = QHEADS // KVH
XS = 4
SLAB_KV = KVH // XS
QW = SLAB_KV * GROUP * HD
KW = SLAB_KV * HD
TOGETHER = 4
REACH = 4
MASKED = -1e30
SCALE = HD**-0.5
EXP2_SCALE = SCALE * 1.4426950408889634
F32 = jnp.float32
BF16 = jnp.bfloat16


def nt(a, b):
    return lax.dot_general(a, b, (((1,), (1,)), ((), ())), preferred_element_type=F32)


def nn(a, b):
    return lax.dot_general(a, b, (((1,), (0,)), ((), ())), preferred_element_type=F32)


def tn(a, b):
    return lax.dot_general(a, b, (((0,), (0,)), ((), ())), preferred_element_type=F32)


def place():
    rank = lax.axis_index("ctx")
    return rank // 2, rank % 2


def vmem_call(body, outs, scratch=(), limit=20):
    return pl.pallas_call(
        body,
        out_shape=outs,
        scratch_shapes=scratch,
        compiler_params=pltpu.CompilerParams(vmem_limit_bytes=limit * 1024 * 1024),
    )


def cut_body(*refs):
    in_refs, (out_ref, held_ref, in_sems, out_sems) = refs[:-4], refs[-4:]
    loads = []
    for slab in range(XS):
        at, row = 0, []
        for n, ref in enumerate(in_refs):
            width = ref.shape[2] // XS
            source = ref.at[0, :, slab * width : (slab + 1) * width]
            target = held_ref.at[slab, :, at : at + width]
            row.append(pltpu.make_async_copy(source, target, in_sems.at[slab, n]))
            at += width
        loads.append(row)
    for row in loads:
        for load in row:
            load.start()
    stores = []
    for slab, row in enumerate(loads):
        for load in row:
            load.wait()
        stores.append(
            pltpu.make_async_copy(held_ref.at[slab], out_ref.at[slab], out_sems.at[slab])
        )
        stores[-1].start()
    for store in stores:
        store.wait()


def cut(*arrays):
    width = sum(a.shape[2] for a in arrays) // XS
    shape = (XS, QBLK, width)
    return pl.pallas_call(
        cut_body,
        in_specs=[pl.BlockSpec(memory_space=pl.ANY)] * len(arrays),
        out_specs=pl.BlockSpec(memory_space=pl.ANY),
        out_shape=jax.ShapeDtypeStruct(shape, BF16),
        scratch_shapes=[
            pltpu.VMEM(shape, BF16),
            pltpu.SemaphoreType.DMA((XS, len(arrays))),
            pltpu.SemaphoreType.DMA((XS,)),
        ],
    )(*arrays)


def turned_body(in_ref, *refs):
    out_refs, sems = refs[:XS], refs[XS]
    x, _ = place()
    width = in_ref.shape[2] // XS
    loads = []
    for k in range(XS):
        start = pl.multiple_of(lax.rem(x + k, XS) * width, width)
        source = in_ref.at[0, :, pl.ds(start, width)]
        loads.append(pltpu.make_async_copy(source, out_refs[k], sems.at[k]))
        loads[-1].start()
    for load in loads:
        load.wait()


def turned(array):
    width = array.shape[2] // XS
    return pl.pallas_call(
        turned_body,
        in_specs=[pl.BlockSpec(memory_space=pl.ANY)],
        out_specs=[pl.BlockSpec(memory_space=pltpu.VMEM)] * XS,
        out_shape=[jax.ShapeDtypeStruct((QBLK, width), BF16)] * XS,
        scratch_shapes=[pltpu.SemaphoreType.DMA((XS,))],
    )(array)


def joined_body(*refs):
    x, _ = place()
    out_ref, width = refs[XS], refs[0].shape[1]
    for k in range(XS):
        start = pl.multiple_of(lax.rem(x - k + XS, XS) * width, width)
        out_ref[0, :, pl.ds(start, width)] = refs[k][...]


def joined(parts):
    width = parts[0].shape[1]
    return vmem_call(joined_body, jax.ShapeDtypeStruct((1, QBLK, XS * width), BF16))(*parts)


def joined_grads_body(*refs):
    x, _ = place()
    mine, theirs, (dq_ref, dk_ref, dv_ref) = refs[:XS], refs[XS : 2 * XS], refs[2 * XS :]
    for k in range(XS):
        slab = lax.rem(x - k + XS, XS)
        wide = pl.multiple_of(slab * QW, QW)
        start = pl.multiple_of(slab * KW, KW)
        dq_ref[0, :, pl.ds(wide, QW)] = mine[k][:, :QW]
        total = mine[k][:, QW:].astype(F32) + theirs[k][...].astype(F32)
        dk_ref[0, :, pl.ds(start, KW)] = total[:, :KW].astype(BF16)
        dv_ref[0, :, pl.ds(start, KW)] = total[:, KW:].astype(BF16)


def joined_grads(mine, theirs):
    shape = jax.ShapeDtypeStruct((1, QBLK, XS * KW), BF16)
    wide = jax.ShapeDtypeStruct((1, QBLK, XS * QW), BF16)
    return vmem_call(joined_grads_body, (wide, shape, shape))(*mine, *theirs)


def sent_turned(parts, steps, flip=0):
    count, outs = lax.axis_size("pipe"), []
    for k in range(XS):
        pairs = []
        for p in range(count):
            for c in range(2 * XS):
                target = (c // 2 + k) % XS * 2 + (c + flip) % 2
                pairs.append((p * 2 * XS + c, (p + steps) % count * 2 * XS + target))
        if all(source == target for source, target in pairs):
            outs.append(parts[k])
            continue
        outs.append(lax.ppermute(parts[k], ("pipe", "ctx"), pairs))
    return outs


def across(value):
    return lax.ppermute(value, "ctx", [(c, c ^ 1) for c in range(2 * XS)])


def over_x(value):
    evens = [2 * x for x in range(XS)]
    odds = [2 * x + 1 for x in range(XS)]
    return lax.all_to_all(
        value, "ctx", split_axis=0, concat_axis=0, axis_index_groups=[evens, odds], tiled=True
    )


def window_of(i, y):
    blocks = min(2 * i + 2, REACH + 1)
    start = 0 if blocks <= REACH else (2 * i - REACH + y)
    return blocks * QBLK, start


def fill_window(y, base, own_ref, other_ref, k_ref, v_ref):
    for i in range(XS):
        own = pl.multiple_of((2 * i + y) * QBLK, QBLK)
        other = pl.multiple_of((2 * i + 1 - y) * QBLK, QBLK)
        k_ref[pl.ds(own, QBLK), :] = own_ref[i, :, base : base + KW]
        v_ref[pl.ds(own, QBLK), :] = own_ref[i, :, base + KW : base + 2 * KW]
        k_ref[pl.ds(other, QBLK), :] = other_ref[i, :, :KW]
        v_ref[pl.ds(other, QBLK), :] = other_ref[i, :, KW:]


def fill_docs(docs_ref, which, col_ref, row_ref):
    for b in range(SEQ // QBLK):
        row = docs_ref[0, which : which + 1, b * QBLK : (b + 1) * QBLK].astype(F32)
        row_ref[b] = jnp.broadcast_to(row, (8, QBLK))
        col_ref[b * QBLK : (b + 1) * QBLK, :] = jnp.broadcast_to(row, (QBLK, QBLK)).T


def fill_bias(i, y, col_ref, row_ref, bias_ref):
    length, start = window_of(i, y)
    first = pl.multiple_of(start * QBLK, QBLK)
    key_docs = col_ref[pl.ds(first, length), :]
    query_docs = row_ref[2 * i + y][:1]
    key_places = first + lax.broadcasted_iota(jnp.int32, (length, QBLK), 0)
    query_places = (2 * i + y) * QBLK + lax.broadcasted_iota(jnp.int32, (length, QBLK), 1)
    seen = (key_places <= query_places) & (key_docs == query_docs)
    bias_ref[:length, :] = jnp.where(seen, F32(0), F32(MASKED))


def stacked(ref, i, first):
    return jnp.concatenate(
        [ref[i, :, h * HD : (h + 1) * HD] for h in range(first, first + TOGETHER)], axis=0
    )


def probs_of(scores, bias):
    masked = scores + jnp.concatenate([bias] * TOGETHER, axis=1)
    row_max = jnp.max(masked, axis=0, keepdims=True)
    exponent = jnp.exp2((masked - row_max) * F32(EXP2_SCALE))
    return exponent * (1.0 / jnp.sum(exponent, axis=0, keepdims=True))


def forward_body(q0, q1, q2, q3, own_ref, other_ref, docs_ref, *refs):
    out_refs, (q_ref, mixed_ref, k_ref, v_ref, col_ref, row_ref, bias_ref) = refs[:XS], refs[XS:]
    x, y = place()
    for k, chunk in enumerate((q0, q1, q2, q3)):
        q_ref[lax.rem(x - k + XS, XS)] = chunk[...]
    fill_window(y, 2 * KW, own_ref, other_ref, k_ref, v_ref)
    fill_docs(docs_ref, 0, col_ref, row_ref)
    for i in range(XS):
        length, start = window_of(i, y)
        first = pl.multiple_of(start * QBLK, QBLK)
        fill_bias(i, y, col_ref, row_ref, bias_ref)
        for head in range(0, SLAB_KV * GROUP, TOGETHER):
            g = head // GROUP
            keys = k_ref[pl.ds(first, length), g * HD : (g + 1) * HD]
            values = v_ref[pl.ds(first, length), g * HD : (g + 1) * HD]
            queries = stacked(q_ref, i, head)
            weights = probs_of(nt(keys, queries), bias_ref[:length, :]).astype(BF16)
            mixed = tn(values, weights)
            for h in range(TOGETHER):
                col = (head + h) * HD
                part = mixed[:, h * QBLK : (h + 1) * QBLK].T
                mixed_ref[i, :, col : col + HD] = part.astype(BF16)
    for k in range(XS):
        out_refs[k][...] = mixed_ref[lax.rem(x + k, XS)]


def forward(q, own, other, docs):
    return vmem_call(
        forward_body,
        (jax.ShapeDtypeStruct((QBLK, QW), BF16),) * XS,
        (
            pltpu.VMEM((XS, QBLK, QW), BF16),
            pltpu.VMEM((XS, QBLK, QW), BF16),
            pltpu.VMEM((SEQ, KW), BF16),
            pltpu.VMEM((SEQ, KW), BF16),
            pltpu.VMEM((SEQ, QBLK), F32),
            pltpu.VMEM((SEQ // QBLK, 8, QBLK), F32),
            pltpu.VMEM(((REACH + 1) * QBLK, QBLK), F32),
        ),
        20,
    )(*q, own, other, docs)


def backward_body(q0, q1, q2, q3, g0, g1, g2, g3, own_ref, other_ref, docs_ref, *refs):
    mine_refs, theirs_refs = refs[:XS], refs[XS : 2 * XS]
    q_ref, g_ref, dq_ref, k_ref, v_ref = refs[2 * XS : 2 * XS + 5]
    col_ref, row_ref, bias_ref, dk_ref, dv_ref = refs[2 * XS + 5 :]
    x, y = place()
    for k, (q_chunk, g_chunk) in enumerate(((q0, g0), (q1, g1), (q2, g2), (q3, g3))):
        q_ref[lax.rem(x - k + XS, XS)] = q_chunk[...]
        g_ref[lax.rem(x - k + XS, XS)] = g_chunk[...]
    fill_window(y, 0, own_ref, other_ref, k_ref, v_ref)
    fill_docs(docs_ref, 1, col_ref, row_ref)
    dk_ref[...] = jnp.zeros_like(dk_ref)
    dv_ref[...] = jnp.zeros_like(dv_ref)
    for i in range(XS):
        length, start = window_of(i, y)
        first = pl.multiple_of(start * QBLK, QBLK)
        fill_bias(i, y, col_ref, row_ref, bias_ref)
        for head in range(0, SLAB_KV * GROUP, TOGETHER):
            g = head // GROUP
            span = (pl.ds(first, length), slice(g * HD, (g + 1) * HD))
            keys, values = k_ref[span], v_ref[span]
            queries = stacked(q_ref, i, head)
            cotan = stacked(g_ref, i, head)
            probs = probs_of(nt(keys, queries), bias_ref[:length, :])
            prob_grad = nt(values, cotan)
            delta = jnp.sum(probs * prob_grad, axis=0, keepdims=True)
            score_grad = (probs * (prob_grad - delta) * F32(SCALE)).astype(BF16)
            dv_ref[span] += nn(probs.astype(BF16), cotan)
            dk_ref[span] += nn(score_grad, queries)
            dq = tn(keys, score_grad)
            for h in range(TOGETHER):
                col = (head + h) * HD
                part = dq[:, h * QBLK : (h + 1) * QBLK].T
                dq_ref[i, :, col : col + HD] = part.astype(BF16)
    for k in range(XS):
        i = lax.rem(x + k, XS)
        own = pl.multiple_of((2 * i + y) * QBLK, QBLK)
        other = pl.multiple_of((2 * i + 1 - y) * QBLK, QBLK)
        mine_refs[k][:, :QW] = dq_ref[i]
        mine_refs[k][:, QW : QW + KW] = dk_ref[pl.ds(own, QBLK), :].astype(BF16)
        mine_refs[k][:, QW + KW :] = dv_ref[pl.ds(own, QBLK), :].astype(BF16)
        theirs_refs[k][:, :KW] = dk_ref[pl.ds(other, QBLK), :].astype(BF16)
        theirs_refs[k][:, KW:] = dv_ref[pl.ds(other, QBLK), :].astype(BF16)


def backward(q, g, own, other, docs):
    outs = vmem_call(
        backward_body,
        (jax.ShapeDtypeStruct((QBLK, QW + 2 * KW), BF16),) * XS
        + (jax.ShapeDtypeStruct((QBLK, 2 * KW), BF16),) * XS,
        (
            pltpu.VMEM((XS, QBLK, QW), BF16),
            pltpu.VMEM((XS, QBLK, QW), BF16),
            pltpu.VMEM((XS, QBLK, QW), BF16),
            pltpu.VMEM((SEQ, KW), BF16),
            pltpu.VMEM((SEQ, KW), BF16),
            pltpu.VMEM((SEQ, QBLK), F32),
            pltpu.VMEM((SEQ // QBLK, 8, QBLK), F32),
            pltpu.VMEM(((REACH + 1) * QBLK, QBLK), F32),
            pltpu.VMEM((SEQ, KW), F32),
            pltpu.VMEM((SEQ, KW), F32),
        ),
        20,
    )(*q, *g, own, other, docs)
    return outs[:XS], outs[XS:]


def shifted(value, steps):
    count = lax.axis_size("pipe")
    return lax.ppermute(value, "pipe", [(p, (p + steps) % count) for p in range(count)])


def on_device(query_fwd, key_fwd, value_fwd, query_bwd, key_bwd, value_bwd, cotangent, documents):
    own = over_x(cut(key_bwd, value_bwd, key_fwd, value_fwd))
    cotan = sent_turned(turned(cotangent), -1)
    queries_bwd = sent_turned(turned(query_bwd), 0)
    kv_bwd = across(own[:, :, : 2 * KW])
    kv_fwd = across(own[:, :, 2 * KW :])
    docs_fwd = shifted(documents, -1)
    queries_fwd = sent_turned(turned(query_fwd), 0)
    mine, theirs = backward(queries_bwd, cotan, own, kv_bwd, documents)
    mine = sent_turned(mine, -1)
    mixed = forward(queries_fwd, own, kv_fwd, docs_fwd)
    mixed = sent_turned(mixed, 1)
    theirs = sent_turned(theirs, -1, 1)
    return joined(mixed), *joined_grads(mine, theirs)


def solution(mesh):
    rows = P("pipe", "ctx", None)
    return jax.shard_map(
        on_device,
        mesh=mesh,
        in_specs=(rows,) * 7 + (P("pipe", None, None),),
        out_specs=(rows,) * 4,
        check_vma=False,
    )
```
